128 devices in a mesh: data: 1, inner: 16 (over z, y), stage: 8 (over x, core).
Axes of the slice: x: 4, y: 4, z: 4, core: 2. Of those that a mesh axis runs over, the one named last changes fastest.
Arguments:
- x_tokens: bfloat16 [128, 32, 1024], P(('data', 'stage', 'inner'))
- g_cotan: bfloat16 [128, 32, 1024], P(('data', 'stage', 'inner'))
- w_up: bfloat16 [2, 8, 1024, 4096], P(None, ('data', 'stage'), None, 'inner')
- w_down: bfloat16 [2, 8, 4096, 1024], P(None, ('data', 'stage'), 'inner')
Outputs:
- output 1: bfloat16 [128, 32, 1024], P(('data', 'stage', 'inner'))
- output 2: bfloat16 [128, 32, 1024], P(('data', 'stage', 'inner'))
- output 3: float32 [2, 8, 1024, 4096], P(None, ('data', 'stage'), None, 'inner')
- output 4: float32 [2, 8, 4096, 1024], P(None, ('data', 'stage'), 'inner')
All inputs are finite; a program needn't handle non-finite values.
Results may differ from the reference program's by a relative error of at most 0.02.
Values are sent between devices in bfloat16 or wider.
A program may use at most 1 GiB of HBM per device.

```python
import jax
import jax.numpy as jnp
from jax import lax

D_MODEL = 1024
D_FF = 4096
MB_TOKENS = 32
MB_PER_DEV = 1
VIRT_STAGES = 2
CHUNK_LAYERS = 1
NUM_STAGES = 8
INNER_SIZE = 16

NUM_MICRO = MB_PER_DEV * NUM_STAGES * INNER_SIZE
STAGE_LAYERS = NUM_STAGES * CHUNK_LAYERS
NUM_LAYERS = VIRT_STAGES * STAGE_LAYERS


def setup_inputs(seed: int = 0, part: int = 0) -> dict:
    base_key = jax.random.fold_in(jax.random.key(seed), part)
    key_list = jax.random.split(base_key, 4)
    tok_shape = (NUM_MICRO, MB_TOKENS, D_MODEL)
    x_tokens = jax.random.normal(key_list[0], tok_shape, jnp.float32)
    g_cotan = jax.random.normal(key_list[1], tok_shape, jnp.float32)
    up_scale = D_MODEL ** -0.5
    down_scale = 1.5 * (D_FF * NUM_LAYERS) ** -0.5
    w_up = jax.random.normal(key_list[2], (VIRT_STAGES, STAGE_LAYERS, D_MODEL, D_FF), jnp.float32) * up_scale
    w_down = jax.random.normal(key_list[3], (VIRT_STAGES, STAGE_LAYERS, D_FF, D_MODEL), jnp.float32) * down_scale
    return {'x_tokens': x_tokens.astype(jnp.bfloat16), 'g_cotan': g_cotan.astype(jnp.bfloat16), 'w_up': w_up.astype(jnp.bfloat16), 'w_down': w_down.astype(jnp.bfloat16)}


def gelu_pair(pre_act):
    normal_cdf = 0.5 * (1.0 + lax.erf(pre_act * 0.7071067811865476))
    normal_pdf = jnp.exp(-0.5 * pre_act * pre_act) * 0.3989422804014327
    return pre_act * normal_cdf, normal_cdf + pre_act * normal_pdf


def reference(x_tokens, g_cotan, w_up, w_down):
    up_layers = w_up.reshape(NUM_LAYERS, D_MODEL, D_FF)
    down_layers = w_down.reshape(NUM_LAYERS, D_FF, D_MODEL)

    def fwd_layer(h_act, weights):
        w_one, w_two = weights
        pre_act = jnp.dot(h_act, w_one, preferred_element_type=jnp.float32)
        act_val = gelu_pair(pre_act)[0].astype(jnp.bfloat16)
        branch = jnp.dot(act_val, w_two, preferred_element_type=jnp.float32)
        h_next = (h_act.astype(jnp.float32) + branch).astype(jnp.bfloat16)
        return h_next, h_act

    def bwd_layer(g_act, layer_items):
        h_in, w_one, w_two = layer_items
        pre_act = jnp.dot(h_in, w_one, preferred_element_type=jnp.float32)
        gelu_val, gelu_grad = gelu_pair(pre_act)
        act_val = gelu_val.astype(jnp.bfloat16)
        d_act = jnp.dot(g_act, w_two.T, preferred_element_type=jnp.float32)
        d_pre = (d_act * gelu_grad).astype(jnp.bfloat16)
        grad_one = jnp.dot(h_in.T, d_pre, preferred_element_type=jnp.float32)
        grad_two = jnp.dot(act_val.T, g_act, preferred_element_type=jnp.float32)
        back_term = jnp.dot(d_pre, w_one.T, preferred_element_type=jnp.float32)
        g_prev = (g_act.astype(jnp.float32) + back_term).astype(jnp.bfloat16)
        return g_prev, (grad_one, grad_two)

    def one_micro(acc_state, micro_items):
        x_micro, g_micro = micro_items
        y_micro, layer_ins = lax.scan(fwd_layer, x_micro, (up_layers, down_layers))
        dx_micro, grad_pair = lax.scan(bwd_layer, g_micro, (layer_ins, up_layers, down_layers), reverse=True)
        new_state = (acc_state[0] + grad_pair[0], acc_state[1] + grad_pair[1])
        return new_state, (y_micro, dx_micro)

    init_state = (jnp.zeros(up_layers.shape, jnp.float32), jnp.zeros(down_layers.shape, jnp.float32))
    final_state, micro_outs = lax.scan(one_micro, init_state, (x_tokens, g_cotan))
    dw_up = final_state[0].reshape(w_up.shape)
    dw_down = final_state[1].reshape(w_down.shape)
    return (micro_outs[0], micro_outs[1], dw_up, dw_down)
```

```python
import functools

import jax
import jax.numpy as jnp
from jax import lax
from jax.experimental import pallas as pl
from jax.experimental.pallas import tpu as pltpu
from jax.sharding import PartitionSpec as P

MESH = pl.DeviceIdType.MESH
NT = (((1,), (1,)), ((), ()))
TN = (((0,), (0,)), ((), ()))
SIDE = 4
CHUNKS = 2
F32 = jnp.float32
BF16 = jnp.bfloat16


def gelu_parts(pre_act):
    normal_cdf = 0.5 * (1.0 + lax.erf(pre_act * 0.7071067811865476))
    normal_pdf = jnp.exp(-0.5 * pre_act * pre_act) * 0.3989422804014327
    return normal_cdf, normal_pdf


def remote(src, dst, send_sem, recv_sem, inner, stage):
    return pltpu.make_async_remote_copy(
        src_ref=src, dst_ref=dst, send_sem=send_sem, recv_sem=recv_sem,
        device_id={'inner': inner, 'stage': stage}, device_id_type=MESH)


class PlaneGather:
    def __init__(self, own, slot, recv_sems, send_sem, inner, stage, y_first):
        self.own, self.slot, self.recv_sems, self.send_sem = own, slot, recv_sems, send_sem
        self.inner, self.stage, self.y_first = inner, stage, y_first
        z_pos, y_pos = lax.div(inner, SIDE), lax.rem(inner, SIDE)
        self.a_pos, self.b_pos = (y_pos, z_pos) if y_first else (z_pos, y_pos)

    def block(self, a_off, b_off):
        a_pos = lax.rem(self.a_pos + a_off + SIDE, SIDE)
        b_pos = lax.rem(self.b_pos + b_off + SIDE, SIDE)
        return b_pos * SIDE + a_pos if self.y_first else a_pos * SIDE + b_pos

    def send(self, block, half, a_off, b_off, sem_idx, own=False):
        src = self.own(half) if own else self.slot(block, half)
        remote(src, self.slot(block, half), self.send_sem, self.recv_sems(sem_idx),
               self.block(a_off, b_off), self.stage).start()

    def wait(self, block, half, sem_idx):
        ref = self.slot(block, half)
        remote(ref, ref, self.send_sem, self.recv_sems(sem_idx), self.inner, self.stage).wait_recv()

    def step_own(self):
        self.send(self.inner, None, 1, 0, 0, own=True)
        self.send(self.inner, None, -1, 0, 1, own=True)

    def step_own_across(self):
        self.send(self.inner, None, 0, 1, 4, own=True)
        self.send(self.inner, None, 0, -1, 5, own=True)

    def step_near(self):
        for side, half in ((-1, 0), (1, 1)):
            block = self.block(side, 0)
            self.wait(block, None, half)
            self.send(block, half, -side, 0, 2 + half)
            for toward in (1, -1):
                self.send(block, None, 0, toward, 4 + 4 * (1 + half) + (0 if toward == 1 else 1))

    def step_far(self):
        block = self.block(2, 0)
        self.wait(block, 0, 2)
        self.wait(block, 1, 3)
        for toward in (1, -1):
            self.send(block, None, 0, toward, 4 + 12 + (0 if toward == 1 else 1))

    def step_relay(self):
        for role, a_off in enumerate((0, -1, 1, 2)):
            for side, half in ((-1, 0), (1, 1)):
                block = self.block(a_off, side)
                self.wait(block, None, 4 + 4 * role + half)
                self.send(block, half, 0, -side, 4 + 4 * role + 2 + half)

    def step_last(self):
        for role, a_off in enumerate((0, -1, 1, 2)):
            block = self.block(a_off, 2)
            for half in (0, 1):
                self.wait(block, half, 4 + 4 * role + 2 + half)

    def step_sent(self, many):
        remote(many, many, self.send_sem, self.recv_sems(0), self.inner, self.stage).wait_send()


class Pair:
    def __init__(self, *parts):
        self.parts = parts

    def __getattr__(self, name):
        def call():
            for part in self.parts:
                getattr(part, name)()
        return call


def main_kernel(n_stage, x_ref, g_ref, wu_ref, wd_ref, y_ref, dx_ref, h_all, g_all,
                w1, w2, zb, act, hb, gb, ho, go,
                load_sem, keep_sem, ag_recv, ag_send, xr, xs, gr, gs, fr, fs, br, bs, yr, ys, dr, ds):
    inner = lax.axis_index('inner')
    stage = lax.axis_index('stage')
    first, last = stage == 0, stage == n_stage - 1
    n_inner = SIDE * SIDE
    n_blk, d_model, f_blk = w1.shape[1:]
    tok = x_ref.shape[1]
    rows = hb.shape[2]
    per_chunk = rows // tok
    half_w1, half_w2 = d_model // 2, f_blk // 2
    half_rows = rows // 2

    loads = []
    for v in range(2):
        loads.append(pltpu.make_async_copy(wu_ref.at[v, 0], w1.at[v, inner], load_sem.at[v, 0]))
        loads.append(pltpu.make_async_copy(wd_ref.at[v, 0], w2.at[v, inner], load_sem.at[v, 1]))
    for load in loads:
        load.start()

    barrier = pltpu.get_barrier_semaphore()
    z_pos, y_pos = lax.div(inner, SIDE), lax.rem(inner, SIDE)
    for off in (1, SIDE - 1):
        for peer in (z_pos * SIDE + lax.rem(y_pos + off, SIDE), lax.rem(z_pos + off, SIDE) * SIDE + y_pos):
            pl.semaphore_signal(barrier, inc=1, device_id={'inner': peer, 'stage': stage}, device_id_type=MESH)
    for off in range(1, n_stage):
        peer = lax.rem(stage + off, n_stage)
        pl.semaphore_signal(barrier, inc=1, device_id={'inner': inner, 'stage': peer}, device_id_type=MESH)
    pl.semaphore_wait(barrier, 4 + n_stage - 1)

    def rows_of(micro):
        return pl.ds(pl.multiple_of(lax.rem(micro, per_chunk) * tok, tok), tok)

    def w_slot(buf, v, half_size):
        def slot(block, half):
            ref = buf.at[v, block]
            return ref if half is None else ref.at[pl.ds(half * half_size, half_size)]
        return slot

    def make_w(v):
        parts = []
        for colour, (buf, half_size) in enumerate(((w1, half_w1), (w2, half_w2))):
            slot = w_slot(buf, v, half_size)
            parts.append(PlaneGather(
                functools.partial(slot, inner), slot, lambda k, u=v, c=colour: ag_recv.at[u, c, k],
                ag_send.at[v, colour], inner, stage, colour == 0))
        return Pair(*parts)

    def make_act(unit, buf, out, v):
        parts = []
        for colour in range(2):
            def own(half, colour=colour):
                ref = buf.at[v, colour]
                return ref if half is None else ref.at[pl.ds(half * half_rows, half_rows)]

            def slot(block, half, colour=colour):
                if half is None:
                    return out.at[v, block, pl.ds(colour * rows, rows)]
                return out.at[v, block, pl.ds(colour * rows + half * half_rows, half_rows)]

            parts.append(PlaneGather(own, slot, lambda k, u=unit, c=colour: ag_recv.at[u, c, k],
                                     ag_send.at[unit, colour], inner, stage, colour == 0))
        return Pair(*parts)

    weights = [make_w(0), make_w(1)]
    acts = [make_act(2, hb, h_all, 0), make_act(3, hb, h_all, 1), make_act(4, gb, g_all, 1), make_act(5, gb, g_all, 0)]

    for v in range(2):
        for load in loads[2 * v:2 * v + 2]:
            load.wait()
        if v == 0:
            weights[0].step_own()
            weights[0].step_own_across()

    chunk = lax.div(stage, per_chunk)
    x_dst = hb.at[0, chunk, rows_of(stage)]
    g_dst = gb.at[1, chunk, rows_of(stage)]

    @pl.when(first)
    def _():
        pltpu.make_async_copy(x_ref.at[0], x_dst, xr.at[stage]).start()

    @pl.when(jnp.logical_not(first))
    def _():
        remote(x_ref.at[0], x_dst, xs.at[0], xr.at[stage], inner, 0).start()

    @pl.when(last)
    def _():
        pltpu.make_async_copy(g_ref.at[0], g_dst, gr.at[stage]).start()

    @pl.when(jnp.logical_not(last))
    def _():
        remote(g_ref.at[0], g_dst, gs.at[0], gr.at[stage], inner, n_stage - 1).start()

    weights[0].step_near()
    weights[0].step_far()
    weights[1].step_own()
    weights[1].step_own_across()
    weights[0].step_relay()
    weights[1].step_near()
    weights[1].step_far()
    weights[0].step_last()

    def wait_in(buf, v, m, ready, micro_ready, from_tokens):
        @pl.when(from_tokens)
        def _():
            for k in range(per_chunk):
                micro = m * per_chunk + k
                ref = buf.at[v, m, pl.ds(k * tok, tok)]
                remote(ref, ref, xs.at[0], micro_ready.at[micro], inner, stage).wait_recv()

        @pl.when(jnp.logical_not(from_tokens))
        def _():
            ref = buf.at[v, m]
            remote(ref, ref, xs.at[0], ready.at[v, m], inner, stage).wait_recv()

    def give_out(buf, v, m, out_ref, sends, recv):
        for k in range(per_chunk):
            micro = m * per_chunk + k
            src = buf.at[v, m, pl.ds(k * tok, tok)]

            @pl.when(micro == stage)
            def _():
                pltpu.make_async_copy(src, out_ref.at[0], recv.at[0]).start()

            @pl.when(micro != stage)
            def _():
                remote(src, out_ref.at[0], sends.at[micro], recv.at[0], inner, micro).start()

    def forward(v, m):
        wait_in(hb, v, m, fr, xr, first & (v == 0))
        h_in = hb[v, m]
        for blk in range(n_blk):
            cols = slice(blk * f_blk, (blk + 1) * f_blk)
            pre_act = jnp.dot(h_in, w1[v, blk], preferred_element_type=F32)
            zb[v, m, :, cols] = pre_act
            normal_cdf = 0.5 * (1.0 + lax.erf(pre_act * 0.7071067811865476))
            act[:, cols] = (pre_act * normal_cdf).astype(BF16)
        branch = jnp.dot(act[...], w2[v].reshape(n_blk * f_blk, d_model), preferred_element_type=F32)
        ho[v, m] = (h_in.astype(F32) + branch).astype(BF16)
        done = last & (v == 1)

        @pl.when(done)
        def _():
            give_out(ho, v, m, y_ref, ys, yr)

        @pl.when(jnp.logical_not(done))
        def _():
            v_to = v + last.astype(jnp.int32)
            remote(ho.at[v, m], hb.at[v_to, m], fs.at[v, m], fr.at[v_to, m], inner,
                   lax.rem(stage + 1, n_stage)).start()

    def backward(v, m):
        wait_in(gb, v, m, br, gr, last & (v == 1))
        g_out = gb[v, m]
        for blk in range(n_blk):
            cols = slice(blk * f_blk, (blk + 1) * f_blk)
            d_act = lax.dot_general(g_out, w2[v, blk], NT, preferred_element_type=F32)
            pre_act = zb[v, m, :, cols]
            normal_cdf, normal_pdf = gelu_parts(pre_act)
            act[:, cols] = (d_act * (normal_cdf + pre_act * normal_pdf)).astype(BF16)
        back = None
        for blk in range(n_blk):
            cols = slice(blk * f_blk, (blk + 1) * f_blk)
            term = lax.dot_general(act[:, cols], w1[v, blk], NT, preferred_element_type=F32)
            back = term if back is None else back + term
        go[v, m] = (g_out.astype(F32) + back).astype(BF16)
        done = first & (v == 0)

        @pl.when(done)
        def _():
            give_out(go, v, m, dx_ref, ds, dr)

        @pl.when(jnp.logical_not(done))
        def _():
            v_to = v - first.astype(jnp.int32)
            remote(go.at[v, m], gb.at[v_to, m], bs.at[v, m], br.at[v_to, m], inner,
                   lax.rem(stage + n_stage - 1, n_stage)).start()

    tail = CHUNKS - 1
    starts = (n_stage,
              jnp.maximum(n_stage + 6, n_stage + stage + tail),
              jnp.maximum(2 * n_stage + 4, 3 * n_stage - 1 - stage + tail),
              jnp.maximum(3 * n_stage + 2, 4 * n_stage - 1 - stage + tail))
    offsets = (('step_own', 0), ('step_own_across', 0), ('step_near', 1), ('step_far', 2), ('step_relay', 4))

    def tick(t, carry):
        ahead = t - stage
        f_pos = jnp.maximum(ahead, 0)
        f_v, f_m = lax.div(f_pos, n_stage), lax.rem(f_pos, n_stage)
        f_on = (ahead >= 0) & (f_v < 2) & (f_m < CHUNKS)
        behind = t - (3 * n_stage - 1) + stage
        b_pos = jnp.maximum(behind, 0)
        b_k, b_m = lax.div(b_pos, n_stage), lax.rem(b_pos, n_stage)
        b_on = (behind >= 0) & (b_k < 2) & (b_m < CHUNKS)

        @pl.when(t == n_stage)
        def _():
            weights[1].step_relay()

        @pl.when(f_on & (f_v == 1) & (f_m == 0))
        def _():
            weights[1].step_last()

        @pl.when(f_on)
        def _():
            forward(f_v, f_m)

        @pl.when(b_on)
        def _():
            backward(1 - b_k, b_m)

        for unit, start in zip(acts, starts):
            for name, off in offsets:
                @pl.when(t == start + off)
                def _():
                    getattr(unit, name)()
        return carry

    lax.fori_loop(0, 4 * n_stage + 7, tick, 0)

    keeps = []
    for k, (buf, out) in enumerate(((hb, h_all), (gb, g_all))):
        for v in range(2):
            for m in range(CHUNKS):
                keeps.append(pltpu.make_async_copy(
                    buf.at[v, m], out.at[v, inner, pl.ds(m * rows, rows)], keep_sem.at[k, v, m]))
    for keep in keeps:
        keep.start()
    for unit in acts:
        unit.step_last()
    for keep in keeps:
        keep.wait()
    for v in range(2):
        for part, buf in zip(weights[v].parts, (w1, w2)):
            part.step_sent(buf.at[v, pl.ds(0, n_inner - 1)])
    for unit, (v, out) in zip(acts, ((0, h_all), (1, h_all), (1, g_all), (0, g_all))):
        for colour, part in enumerate(unit.parts):
            part.step_sent(out.at[v, pl.ds(0, n_inner - 1), pl.ds(colour * rows, rows)])

    def wait_sent(ref, sem):
        remote(ref, ref, sem, xr.at[0], inner, stage).wait_send()

    @pl.when(jnp.logical_not(first))
    def _():
        wait_sent(x_ref.at[0], xs.at[0])

    @pl.when(jnp.logical_not(last))
    def _():
        wait_sent(g_ref.at[0], gs.at[0])

    for v in range(2):
        for m in range(CHUNKS):
            @pl.when(jnp.logical_not(last & (v == 1)))
            def _():
                wait_sent(ho.at[v, m], fs.at[v, m])

            @pl.when(jnp.logical_not(first & (v == 0)))
            def _():
                wait_sent(go.at[v, m], bs.at[v, m])

    for micro in range(n_stage):
        @pl.when(last & (stage != micro))
        def _():
            wait_sent(ho.at[1, 0, pl.ds(0, tok)], ys.at[micro])

        @pl.when(first & (stage != micro))
        def _():
            wait_sent(go.at[0, 0, pl.ds(0, tok)], ds.at[micro])

    remote(y_ref.at[0], y_ref.at[0], xs.at[0], yr.at[0], inner, stage).wait_recv()
    remote(dx_ref.at[0], dx_ref.at[0], xs.at[0], dr.at[0], inner, stage).wait_recv()


def grad_kernel(h_ref, g_ref, wu_ref, wd_ref, du_ref, dd_ref, acc):
    step = pl.program_id(1)

    @pl.when(step == 0)
    def _():
        acc[...] = jnp.zeros_like(acc)
        dd_ref[...] = jnp.zeros_like(dd_ref)

    h_in, g_out = h_ref[0], g_ref[0]
    pre_act = jnp.dot(h_in, wu_ref[0, 0], preferred_element_type=F32)
    d_act = lax.dot_general(g_out, wd_ref[0, 0], NT, preferred_element_type=F32)
    normal_cdf, normal_pdf = gelu_parts(pre_act)
    act_val = (pre_act * normal_cdf).astype(BF16)
    d_pre = (d_act * (normal_cdf + pre_act * normal_pdf)).astype(BF16)
    acc[...] += lax.dot_general(d_pre, h_in, TN, preferred_element_type=F32)
    dd_ref[0, 0] += lax.dot_general(act_val, g_out, TN, preferred_element_type=F32)

    @pl.when(step == pl.num_programs(1) - 1)
    def _():
        du_ref[0, 0] = acc[...].T


def solution(mesh):
    n_stage = mesh.shape['stage']
    n_inner = mesh.shape['inner']
    tok_spec = P(('data', 'stage', 'inner'))
    up_spec = P(None, ('data', 'stage'), None, 'inner')
    down_spec = P(None, ('data', 'stage'), 'inner', None)

    def device_step(x_loc, g_loc, w_up, w_down):
        tok, d_model = x_loc.shape[1:]
        f_blk = w_up.shape[3]
        rows = n_stage * tok // CHUNKS
        lane = n_stage * tok
        f_full = n_inner * f_blk
        any_spec = pl.BlockSpec(memory_space=pl.ANY)
        dma = pltpu.SemaphoreType.DMA
        y_loc, dx_loc, h_all, g_all = pl.pallas_call(
            functools.partial(main_kernel, n_stage),
            name='stack',
            out_shape=(jax.ShapeDtypeStruct(x_loc.shape, BF16), jax.ShapeDtypeStruct(x_loc.shape, BF16),
                       jax.ShapeDtypeStruct((2, n_inner, lane, d_model), BF16),
                       jax.ShapeDtypeStruct((2, n_inner, lane, d_model), BF16)),
            in_specs=[any_spec] * 4,
            out_specs=(any_spec,) * 4,
            scratch_shapes=[
                pltpu.VMEM((2, n_inner, d_model, f_blk), BF16),
                pltpu.VMEM((2, n_inner, f_blk, d_model), BF16),
                pltpu.VMEM((2, CHUNKS, rows, f_full), F32),
                pltpu.VMEM((rows, f_full), BF16),
                pltpu.VMEM((2, CHUNKS, rows, d_model), BF16),
                pltpu.VMEM((2, CHUNKS, rows, d_model), BF16),
                pltpu.VMEM((2, CHUNKS, rows, d_model), BF16),
                pltpu.VMEM((2, CHUNKS, rows, d_model), BF16),
                dma((2, 2)), dma((2, 2, CHUNKS)), dma((6, 2, 20)), dma((6, 2)),
                dma((n_stage,)), dma((1,)), dma((n_stage,)), dma((1,)),
                dma((2, CHUNKS)), dma((2, CHUNKS)), dma((2, CHUNKS)), dma((2, CHUNKS)),
                dma((1,)), dma((n_stage,)), dma((1,)), dma((n_stage,)),
            ],
            compiler_params=pltpu.CompilerParams(
                collective_id=0, has_side_effects=True, vmem_limit_bytes=60 << 20),
        )(x_loc, g_loc, w_up, w_down)

        tokens = n_inner * lane
        blk = min(512, tokens)
        h_all = h_all.reshape(2, tokens, d_model)
        g_all = g_all.reshape(2, tokens, d_model)
        dw_up, dw_down = pl.pallas_call(
            grad_kernel,
            name='grads',
            grid=(2, tokens // blk),
            out_shape=(jax.ShapeDtypeStruct(w_up.shape, F32), jax.ShapeDtypeStruct(w_down.shape, F32)),
            in_specs=[pl.BlockSpec((1, blk, d_model), lambda v, t: (v, t, 0)),
                      pl.BlockSpec((1, blk, d_model), lambda v, t: (v, t, 0)),
                      pl.BlockSpec((1, 1, d_model, f_blk), lambda v, t: (v, 0, 0, 0)),
                      pl.BlockSpec((1, 1, f_blk, d_model), lambda v, t: (v, 0, 0, 0))],
            out_specs=(pl.BlockSpec((1, 1, d_model, f_blk), lambda v, t: (v, 0, 0, 0)),
                       pl.BlockSpec((1, 1, f_blk, d_model), lambda v, t: (v, 0, 0, 0))),
            scratch_shapes=[pltpu.VMEM((f_blk, d_model), F32)],
            compiler_params=pltpu.CompilerParams(
                dimension_semantics=('arbitrary', 'arbitrary'), vmem_limit_bytes=40 << 20),
        )(h_all, g_all, w_up, w_down)
        return y_loc, dx_loc, dw_up, dw_down

    return jax.shard_map(device_step, mesh=mesh, in_specs=(tok_spec, tok_spec, up_spec, down_spec),
                         out_specs=(tok_spec, tok_spec, up_spec, down_spec), check_vma=False)
```

```python
import functools

import jax
import jax.numpy as jnp
from jax import lax
from jax.experimental import pallas as pl
from jax.experimental.pallas import tpu as pltpu
from jax.sharding import PartitionSpec as P

MESH = pl.DeviceIdType.MESH
NT = (((1,), (1,)), ((), ()))
TN = (((0,), (0,)), ((), ()))
SIDE = 4
CHUNKS = 2
F32 = jnp.float32
BF16 = jnp.bfloat16


def gelu_parts(pre_act):
    normal_cdf = 0.5 * (1.0 + lax.erf(pre_act * 0.7071067811865476))
    normal_pdf = jnp.exp(-0.5 * pre_act * pre_act) * 0.3989422804014327
    return normal_cdf, normal_pdf


def remote(src, dst, send_sem, recv_sem, inner, stage):
    return pltpu.make_async_remote_copy(
        src_ref=src, dst_ref=dst, send_sem=send_sem, recv_sem=recv_sem,
        device_id={'inner': inner, 'stage': stage}, device_id_type=MESH)


class PlaneGather:
    def __init__(self, own, slot, recv_sems, send_sem, inner, stage, y_first):
        self.own, self.slot, self.recv_sems, self.send_sem = own, slot, recv_sems, send_sem
        self.inner, self.stage, self.y_first = inner, stage, y_first
        z_pos, y_pos = lax.div(inner, SIDE), lax.rem(inner, SIDE)
        self.a_pos, self.b_pos = (y_pos, z_pos) if y_first else (z_pos, y_pos)

    def block(self, a_off, b_off):
        a_pos = lax.rem(self.a_pos + a_off + SIDE, SIDE)
        b_pos = lax.rem(self.b_pos + b_off + SIDE, SIDE)
        return b_pos * SIDE + a_pos if self.y_first else a_pos * SIDE + b_pos

    def send(self, block, half, a_off, b_off, sem_idx, own=False):
        src = self.own(half) if own else self.slot(block, half)
        remote(src, self.slot(block, half), self.send_sem, self.recv_sems(sem_idx),
               self.block(a_off, b_off), self.stage).start()

    def wait(self, block, half, sem_idx):
        ref = self.slot(block, half)
        remote(ref, ref, self.send_sem, self.recv_sems(sem_idx), self.inner, self.stage).wait_recv()

    def step_own(self):
        self.send(self.inner, None, 1, 0, 0, own=True)
        self.send(self.inner, None, -1, 0, 1, own=True)

    def step_own_across(self):
        self.send(self.inner, None, 0, 1, 4, own=True)
        self.send(self.inner, None, 0, -1, 5, own=True)

    def step_near(self):
        for side, half in ((-1, 0), (1, 1)):
            block = self.block(side, 0)
            self.wait(block, None, half)
            self.send(block, half, -side, 0, 2 + half)
            for toward in (1, -1):
                self.send(block, None, 0, toward, 4 + 4 * (1 + half) + (0 if toward == 1 else 1))

    def step_far(self):
        block = self.block(2, 0)
        self.wait(block, 0, 2)
        self.wait(block, 1, 3)
        for toward in (1, -1):
            self.send(block, None, 0, toward, 4 + 12 + (0 if toward == 1 else 1))

    def step_relay(self):
        for role, a_off in enumerate((0, -1, 1, 2)):
            for side, half in ((-1, 0), (1, 1)):
                block = self.block(a_off, side)
                self.wait(block, None, 4 + 4 * role + half)
                self.send(block, half, 0, -side, 4 + 4 * role + 2 + half)

    def step_last(self):
        for role, a_off in enumerate((0, -1, 1, 2)):
            block = self.block(a_off, 2)
            for half in (0, 1):
                self.wait(block, half, 4 + 4 * role + 2 + half)

    def step_sent(self, many):
        remote(many, many, self.send_sem, self.recv_sems(0), self.inner, self.stage).wait_send()


class Pair:
    def __init__(self, *parts):
        self.parts = parts

    def __getattr__(self, name):
        def call():
            for part in self.parts:
                getattr(part, name)()
        return call


def main_kernel(n_stage, x_ref, g_ref, wu_ref, wd_ref, y_ref, dx_ref, h_all, g_all,
                w1, w2, zb, act, hb, gb, ho, go,
                load_sem, keep_sem, ag_recv, ag_send, xr, xs, gr, gs, fr, fs, br, bs, yr, ys, dr, ds):
    inner = lax.axis_index('inner')
    stage = lax.axis_index('stage')
    first, last = stage == 0, stage == n_stage - 1
    n_inner = SIDE * SIDE
    n_blk, n_tile, f_blk = w1.shape[1:4]
    d_model = n_tile * f_blk
    tok = x_ref.shape[1]
    rows = hb.shape[2]
    per_chunk = rows // tok
    half_tiles = n_tile // 2
    half_rows = rows // 2

    loads = []
    for v in range(2):
        for k in range(n_tile):
            part = pl.ds(k * f_blk, f_blk)
            loads.append(pltpu.make_async_copy(wu_ref.at[v, 0, part], w1.at[v, inner, k], load_sem.at[v, 0, k]))
            loads.append(pltpu.make_async_copy(wd_ref.at[v, 0, :, part], w2.at[v, inner, k], load_sem.at[v, 1, k]))
    for load in loads:
        load.start()

    barrier = pltpu.get_barrier_semaphore()
    z_pos, y_pos = lax.div(inner, SIDE), lax.rem(inner, SIDE)
    for off in (1, SIDE - 1):
        for peer in (z_pos * SIDE + lax.rem(y_pos + off, SIDE), lax.rem(z_pos + off, SIDE) * SIDE + y_pos):
            pl.semaphore_signal(barrier, inc=1, device_id={'inner': peer, 'stage': stage}, device_id_type=MESH)
    for off in range(1, n_stage):
        peer = lax.rem(stage + off, n_stage)
        pl.semaphore_signal(barrier, inc=1, device_id={'inner': inner, 'stage': peer}, device_id_type=MESH)
    pl.semaphore_wait(barrier, 4 + n_stage - 1)

    def rows_of(micro):
        return pl.ds(pl.multiple_of(lax.rem(micro, per_chunk) * tok, tok), tok)

    def w_slot(buf, v, half_size):
        def slot(block, half):
            ref = buf.at[v, block]
            return ref if half is None else ref.at[pl.ds(half * half_size, half_size)]
        return slot

    def make_w(v):
        parts = []
        for colour, (buf, half_size) in enumerate(((w1, half_tiles), (w2, half_tiles))):
            slot = w_slot(buf, v, half_size)
            parts.append(PlaneGather(
                functools.partial(slot, inner), slot, lambda k, u=v, c=colour: ag_recv.at[u, c, k],
                ag_send.at[v, colour], inner, stage, colour == 0))
        return Pair(*parts)

    def make_act(unit, buf, out, v):
        parts = []
        for colour in range(2):
            def own(half, colour=colour):
                ref = buf.at[v, colour]
                return ref if half is None else ref.at[pl.ds(half * half_rows, half_rows)]

            def slot(block, half, colour=colour):
                if half is None:
                    return out.at[v, block, pl.ds(colour * rows, rows)]
                return out.at[v, block, pl.ds(colour * rows + half * half_rows, half_rows)]

            parts.append(PlaneGather(own, slot, lambda k, u=unit, c=colour: ag_recv.at[u, c, k],
                                     ag_send.at[unit, colour], inner, stage, colour == 0))
        return Pair(*parts)

    weights = [make_w(0), make_w(1)]
    acts = [make_act(2, hb, h_all, 0), make_act(3, hb, h_all, 1), make_act(4, gb, g_all, 1), make_act(5, gb, g_all, 0)]

    for v in range(2):
        for load in loads[2 * n_tile * v:2 * n_tile * (v + 1)]:
            load.wait()
        if v == 0:
            weights[0].step_own()
            weights[0].step_own_across()

    chunk = lax.div(stage, per_chunk)
    x_dst = hb.at[0, chunk, rows_of(stage)]
    g_dst = gb.at[1, chunk, rows_of(stage)]

    @pl.when(first)
    def _():
        pltpu.make_async_copy(x_ref.at[0], x_dst, xr.at[stage]).start()

    @pl.when(jnp.logical_not(first))
    def _():
        remote(x_ref.at[0], x_dst, xs.at[0], xr.at[stage], inner, 0).start()

    @pl.when(last)
    def _():
        pltpu.make_async_copy(g_ref.at[0], g_dst, gr.at[stage]).start()

    @pl.when(jnp.logical_not(last))
    def _():
        remote(g_ref.at[0], g_dst, gs.at[0], gr.at[stage], inner, n_stage - 1).start()

    weights[0].step_near()
    weights[0].step_far()
    weights[1].step_own()
    weights[1].step_own_across()
    weights[0].step_relay()
    weights[1].step_near()
    weights[0].step_last()

    def wait_in(buf, v, m, ready, micro_ready, from_tokens):
        @pl.when(from_tokens)
        def _():
            for k in range(per_chunk):
                micro = m * per_chunk + k
                ref = buf.at[v, m, pl.ds(k * tok, tok)]
                remote(ref, ref, xs.at[0], micro_ready.at[micro], inner, stage).wait_recv()

        @pl.when(jnp.logical_not(from_tokens))
        def _():
            ref = buf.at[v, m]
            remote(ref, ref, xs.at[0], ready.at[v, m], inner, stage).wait_recv()

    def give_out(buf, v, m, out_ref, sends, recv):
        for k in range(per_chunk):
            micro = m * per_chunk + k
            src = buf.at[v, m, pl.ds(k * tok, tok)]

            @pl.when(micro == stage)
            def _():
                pltpu.make_async_copy(src, out_ref.at[0], recv.at[0]).start()

            @pl.when(micro != stage)
            def _():
                remote(src, out_ref.at[0], sends.at[micro], recv.at[0], inner, micro).start()

    def forward(v, m):
        wait_in(hb, v, m, fr, xr, first & (v == 0))
        h_in = hb[v, m]
        for blk in range(n_blk):
            cols = slice(blk * f_blk, (blk + 1) * f_blk)
            pre_act = jnp.dot(h_in, w1[v, blk].reshape(d_model, f_blk), preferred_element_type=F32)
            zb[v, m, :, cols] = pre_act
            normal_cdf = 0.5 * (1.0 + lax.erf(pre_act * 0.7071067811865476))
            act[:, cols] = (pre_act * normal_cdf).astype(BF16)
        for k in range(n_tile):
            cols = slice(k * f_blk, (k + 1) * f_blk)
            branch = jnp.dot(act[...], w2[v, :, k].reshape(n_blk * f_blk, f_blk), preferred_element_type=F32)
            ho[v, m, :, cols] = (hb[v, m, :, cols].astype(F32) + branch).astype(BF16)
        done = last & (v == 1)

        @pl.when(done)
        def _():
            give_out(ho, v, m, y_ref, ys, yr)

        @pl.when(jnp.logical_not(done))
        def _():
            v_to = v + last.astype(jnp.int32)
            remote(ho.at[v, m], hb.at[v_to, m], fs.at[v, m], fr.at[v_to, m], inner,
                   lax.rem(stage + 1, n_stage)).start()

    def transpose(v):
        for u in range(2):
            @pl.when(v == u)
            def _():
                for part, buf in zip(weights[u].parts, (w1, w2)):
                    part.step_sent(buf.at[u, pl.ds(0, n_inner - 1)])

        def tiles(blk, carry):
            for buf in (w2, w1):
                for k in range(n_tile):
                    buf[v, blk, k] = buf[v, blk, k].T
            return carry

        lax.fori_loop(0, n_blk, tiles, 0)

    def backward(v, m):
        wait_in(gb, v, m, br, gr, last & (v == 1))
        g_out = gb[v, m]
        for blk in range(n_blk):
            cols = slice(blk * f_blk, (blk + 1) * f_blk)
            d_act = jnp.dot(g_out, w2[v, blk].reshape(d_model, f_blk), preferred_element_type=F32)
            pre_act = zb[v, m, :, cols]
            normal_cdf, normal_pdf = gelu_parts(pre_act)
            act[:, cols] = (d_act * (normal_cdf + pre_act * normal_pdf)).astype(BF16)
        for k in range(n_tile):
            cols = slice(k * f_blk, (k + 1) * f_blk)
            back = jnp.dot(act[...], w1[v, :, k].reshape(n_blk * f_blk, f_blk), preferred_element_type=F32)
            go[v, m, :, cols] = (gb[v, m, :, cols].astype(F32) + back).astype(BF16)
        done = first & (v == 0)

        @pl.when(done)
        def _():
            give_out(go, v, m, dx_ref, ds, dr)

        @pl.when(jnp.logical_not(done))
        def _():
            v_to = v - first.astype(jnp.int32)
            remote(go.at[v, m], gb.at[v_to, m], bs.at[v, m], br.at[v_to, m], inner,
                   lax.rem(stage + n_stage - 1, n_stage)).start()

    tail = CHUNKS - 1
    starts = (n_stage,
              jnp.maximum(n_stage + 6, n_stage + stage + tail),
              jnp.maximum(2 * n_stage + 4, 3 * n_stage - 1 - stage + tail),
              jnp.maximum(3 * n_stage + 2, 4 * n_stage - 1 - stage + tail))
    offsets = (('step_own', 0), ('step_own_across', 0), ('step_near', 1), ('step_far', 2), ('step_relay', 4))

    def tick(t, carry):
        ahead = t - stage
        f_pos = jnp.maximum(ahead, 0)
        f_v, f_m = lax.div(f_pos, n_stage), lax.rem(f_pos, n_stage)
        f_on = (ahead >= 0) & (f_v < 2) & (f_m < CHUNKS)
        behind = t - (3 * n_stage - 1) + stage
        b_pos = jnp.maximum(behind, 0)
        b_k, b_m = lax.div(b_pos, n_stage), lax.rem(b_pos, n_stage)
        b_on = (behind >= 0) & (b_k < 2) & (b_m < CHUNKS)

        @pl.when(t == CHUNKS)
        def _():
            weights[1].step_far()

        @pl.when(t == n_stage)
        def _():
            weights[1].step_relay()

        @pl.when(f_on & (f_v == 1) & (f_m == 0))
        def _():
            weights[1].step_last()

        @pl.when(f_on)
        def _():
            forward(f_v, f_m)

        @pl.when(f_on & (f_m == CHUNKS - 1))
        def _():
            transpose(f_v)

        @pl.when(b_on)
        def _():
            backward(1 - b_k, b_m)

        for unit, start in zip(acts, starts):
            for name, off in offsets:
                @pl.when(t == start + off)
                def _():
                    getattr(unit, name)()
        return carry

    lax.fori_loop(0, 4 * n_stage + 7, tick, 0)

    keeps = []
    for k, (buf, out) in enumerate(((hb, h_all), (gb, g_all))):
        for v in range(2):
            for m in range(CHUNKS):
                keeps.append(pltpu.make_async_copy(
                    buf.at[v, m], out.at[v, inner, pl.ds(m * rows, rows)], keep_sem.at[k, v, m]))
    for keep in keeps:
        keep.start()
    for unit in acts:
        unit.step_last()
    for keep in keeps:
        keep.wait()
    for unit, (v, out) in zip(acts, ((0, h_all), (1, h_all), (1, g_all), (0, g_all))):
        for colour, part in enumerate(unit.parts):
            part.step_sent(out.at[v, pl.ds(0, n_inner - 1), pl.ds(colour * rows, rows)])

    def wait_sent(ref, sem):
        remote(ref, ref, sem, xr.at[0], inner, stage).wait_send()

    @pl.when(jnp.logical_not(first))
    def _():
        wait_sent(x_ref.at[0], xs.at[0])

    @pl.when(jnp.logical_not(last))
    def _():
        wait_sent(g_ref.at[0], gs.at[0])

    for v in range(2):
        for m in range(CHUNKS):
            @pl.when(jnp.logical_not(last & (v == 1)))
            def _():
                wait_sent(ho.at[v, m], fs.at[v, m])

            @pl.when(jnp.logical_not(first & (v == 0)))
            def _():
                wait_sent(go.at[v, m], bs.at[v, m])

    for micro in range(n_stage):
        @pl.when(last & (stage != micro))
        def _():
            wait_sent(ho.at[1, 0, pl.ds(0, tok)], ys.at[micro])

        @pl.when(first & (stage != micro))
        def _():
            wait_sent(go.at[0, 0, pl.ds(0, tok)], ds.at[micro])

    remote(y_ref.at[0], y_ref.at[0], xs.at[0], yr.at[0], inner, stage).wait_recv()
    remote(dx_ref.at[0], dx_ref.at[0], xs.at[0], dr.at[0], inner, stage).wait_recv()


def grad_kernel(h_ref, g_ref, wu_ref, wd_ref, du_ref, dd_ref, acc):
    step = pl.program_id(1)

    @pl.when(step == 0)
    def _():
        acc[...] = jnp.zeros_like(acc)
        dd_ref[...] = jnp.zeros_like(dd_ref)

    h_in, g_out = h_ref[0], g_ref[0]
    pre_act = jnp.dot(h_in, wu_ref[0, 0], preferred_element_type=F32)
    d_act = lax.dot_general(g_out, wd_ref[0, 0], NT, preferred_element_type=F32)
    normal_cdf, normal_pdf = gelu_parts(pre_act)
    act_val = (pre_act * normal_cdf).astype(BF16)
    d_pre = (d_act * (normal_cdf + pre_act * normal_pdf)).astype(BF16)
    acc[...] += lax.dot_general(d_pre, h_in, TN, preferred_element_type=F32)
    dd_ref[0, 0] += lax.dot_general(act_val, g_out, TN, preferred_element_type=F32)

    @pl.when(step == pl.num_programs(1) - 1)
    def _():
        du_ref[0, 0] = acc[...].T


def solution(mesh):
    n_stage = mesh.shape['stage']
    n_inner = mesh.shape['inner']
    tok_spec = P(('data', 'stage', 'inner'))
    up_spec = P(None, ('data', 'stage'), None, 'inner')
    down_spec = P(None, ('data', 'stage'), 'inner', None)

    def device_step(x_loc, g_loc, w_up, w_down):
        tok, d_model = x_loc.shape[1:]
        f_blk = w_up.shape[3]
        rows = n_stage * tok // CHUNKS
        lane = n_stage * tok
        f_full = n_inner * f_blk
        any_spec = pl.BlockSpec(memory_space=pl.ANY)
        dma = pltpu.SemaphoreType.DMA
        y_loc, dx_loc, h_all, g_all = pl.pallas_call(
            functools.partial(main_kernel, n_stage),
            name='stack',
            out_shape=(jax.ShapeDtypeStruct(x_loc.shape, BF16), jax.ShapeDtypeStruct(x_loc.shape, BF16),
                       jax.ShapeDtypeStruct((2, n_inner, lane, d_model), BF16),
                       jax.ShapeDtypeStruct((2, n_inner, lane, d_model), BF16)),
            in_specs=[any_spec] * 4,
            out_specs=(any_spec,) * 4,
            scratch_shapes=[
                pltpu.VMEM((2, n_inner, d_model // f_blk, f_blk, f_blk), BF16),
                pltpu.VMEM((2, n_inner, d_model // f_blk, f_blk, f_blk), BF16),
                pltpu.VMEM((2, CHUNKS, rows, f_full), F32),
                pltpu.VMEM((rows, f_full), BF16),
                pltpu.VMEM((2, CHUNKS, rows, d_model), BF16),
                pltpu.VMEM((2, CHUNKS, rows, d_model), BF16),
                pltpu.VMEM((2, CHUNKS, rows, d_model), BF16),
                pltpu.VMEM((2, CHUNKS, rows, d_model), BF16),
                dma((2, 2, d_model // f_blk)), dma((2, 2, CHUNKS)), dma((6, 2, 20)), dma((6, 2)),
                dma((n_stage,)), dma((1,)), dma((n_stage,)), dma((1,)),
                dma((2, CHUNKS)), dma((2, CHUNKS)), dma((2, CHUNKS)), dma((2, CHUNKS)),
                dma((1,)), dma((n_stage,)), dma((1,)), dma((n_stage,)),
            ],
            compiler_params=pltpu.CompilerParams(
                collective_id=0, has_side_effects=True, vmem_limit_bytes=60 << 20),
        )(x_loc, g_loc, w_up, w_down)

        tokens = n_inner * lane
        blk = min(512, tokens)
        h_all = h_all.reshape(2, tokens, d_model)
        g_all = g_all.reshape(2, tokens, d_model)
        dw_up, dw_down = pl.pallas_call(
            grad_kernel,
            name='grads',
            grid=(2, tokens // blk),
            out_shape=(jax.ShapeDtypeStruct(w_up.shape, F32), jax.ShapeDtypeStruct(w_down.shape, F32)),
            in_specs=[pl.BlockSpec((1, blk, d_model), lambda v, t: (v, t, 0)),
                      pl.BlockSpec((1, blk, d_model), lambda v, t: (v, t, 0)),
                      pl.BlockSpec((1, 1, d_model, f_blk), lambda v, t: (v, 0, 0, 0)),
                      pl.BlockSpec((1, 1, f_blk, d_model), lambda v, t: (v, 0, 0, 0))],
            out_specs=(pl.BlockSpec((1, 1, d_model, f_blk), lambda v, t: (v, 0, 0, 0)),
                       pl.BlockSpec((1, 1, f_blk, d_model), lambda v, t: (v, 0, 0, 0))),
            scratch_shapes=[pltpu.VMEM((f_blk, d_model), F32)],
            compiler_params=pltpu.CompilerParams(
                dimension_semantics=('arbitrary', 'arbitrary'), vmem_limit_bytes=40 << 20),
        )(h_all, g_all, w_up, w_down)
        return y_loc, dx_loc, dw_up, dw_down

    return jax.shard_map(device_step, mesh=mesh, in_specs=(tok_spec, tok_spec, up_spec, down_spec),
                         out_specs=(tok_spec, tok_spec, up_spec, down_spec), check_vma=False)
```

```python
import functools

import jax
import jax.numpy as jnp
from jax import lax
from jax.experimental import pallas as pl
from jax.experimental.pallas import tpu as pltpu
from jax.sharding import PartitionSpec as P

MESH = pl.DeviceIdType.MESH
NT = (((1,), (1,)), ((), ()))
TN = (((0,), (0,)), ((), ()))
SIDE = 4
F32 = jnp.float32
BF16 = jnp.bfloat16


def gelu_parts(pre_act):
    normal_cdf = 0.5 * (1.0 + lax.erf(pre_act * 0.7071067811865476))
    normal_pdf = jnp.exp(-0.5 * pre_act * pre_act) * 0.3989422804014327
    return normal_cdf, normal_pdf


class Place:
    def __init__(self, n_stage):
        inner, stage = lax.axis_index('inner'), lax.axis_index('stage')
        self.n_x = n_stage // 2
        self.z, self.y = lax.div(inner, SIDE), lax.rem(inner, SIDE)
        self.x, self.core = lax.div(stage, 2), lax.rem(stage, 2)
        self.column = lax.div(self.y, 2)
        self.role = lax.rem(self.column + self.x, 2)
        self.level = 2 * self.x + self.role
        self.key = jnp.where(self.y < 2, self.y, 3 - self.y)
        self.pair_y = self.y + 1 - 2 * lax.rem(self.y, 2)
        self.mate_y = 3 - self.y

    def at(self, x=None, y=None, z=None, core=None):
        x, y = self.x if x is None else x, self.y if y is None else y
        z, core = self.z if z is None else z, self.core if core is None else core
        return {'inner': z * SIDE + y, 'stage': x * 2 + core}

    def z_off(self, off):
        return lax.rem(self.z + off + SIDE, SIDE)


def remote(src, dst, send_sem, recv_sem, where):
    return pltpu.make_async_remote_copy(src_ref=src, dst_ref=dst, send_sem=send_sem, recv_sem=recv_sem,
                                        device_id=where, device_id_type=MESH)


class Gather:
    def __init__(self, place, core, slot, own, arrive, share, ici_sem, d2d_sem):
        self.place, self.core, self.slot, self.own = place, core, slot, own
        self.arrive, self.share, self.ici_sem, self.d2d_sem = arrive, share, ici_sem, d2d_sem

    def piece(self, d_z, d_k):
        place = self.place
        return place.z_off((0, -1, 1, 2)[d_z]), place.key if d_k == 0 else 1 - place.key

    def ref(self, d_z, d_k, half=None):
        if d_z == 0 and d_k == 0:
            return self.own(half)
        return self.slot(*self.piece(d_z, d_k), half)

    def send(self, d_z, d_k, half, where, as_z, as_k):
        sem = self.arrive((as_z * 2 + as_k) * 2 + (half or 0))
        remote(self.ref(d_z, d_k, half), self.slot(*self.piece(d_z, d_k), half), self.ici_sem, sem, where).start()

    def to_pair(self, d_z, half=None):
        self.send(d_z, 0, half, self.place.at(y=self.place.pair_y), d_z, 1)

    def to_z(self, d_k, up):
        self.send(0, d_k, None, self.place.at(z=self.place.z_off(1 if up else -1)), 1 if up else 2, d_k)

    def across_z(self, d_z, d_k):
        half, off = (0, 1) if d_z == 1 else (1, -1)
        self.send(d_z, d_k, half, self.place.at(z=self.place.z_off(off)), 3, d_k)

    def wait(self, d_z, d_k, half=None):
        ref = self.slot(*self.piece(d_z, d_k), half)
        sem = self.arrive((d_z * 2 + d_k) * 2 + (half or 0))
        remote(ref, ref, self.ici_sem, sem, self.place.at()).wait_recv()

    def pass_on(self, d_z, d_k, half=None):
        sem = self.share((d_z * 2 + d_k) * 2 + (half or 0))
        remote(self.ref(d_z, d_k, half), self.slot(*self.piece(d_z, d_k), half), self.d2d_sem, sem,
               self.place.at(core=1 - self.place.core)).start()

    def start(self):
        if self.core == 0:
            self.to_pair(0)
            self.to_z(0, True)
            self.to_z(0, False)
        else:
            self.to_z(0, True)
            self.to_z(0, False)
            self.to_pair(0)

    def near(self):
        if self.core == 0:
            self.wait(0, 1)
            self.to_z(1, True)
            self.to_z(1, False)
            self.pass_on(0, 1)
        else:
            for d_z in (1, 2):
                self.wait(d_z, 0)
                self.across_z(d_z, 0)
                self.to_pair(d_z)
                self.pass_on(d_z, 0)

    def relay(self):
        if self.core == 0:
            for d_k in (0, 1):
                for d_z in (1, 2):
                    self.wait(d_z, d_k)
                    self.across_z(d_z, d_k)
                    self.pass_on(d_z, d_k)
        else:
            for half in (0, 1):
                self.wait(3, 0, half)
            self.to_pair(3)
            self.pass_on(3, 0)

    def last(self):
        if self.core == 0:
            for d_k in (0, 1):
                for half in (0, 1):
                    self.wait(3, d_k, half)
                    self.pass_on(3, d_k, half)
        else:
            for d_z in range(4):
                self.wait(d_z, 1)
                self.pass_on(d_z, 1)

    def shared(self):
        for d_z in range(4):
            for d_k in range(2):
                if d_z == 0 and d_k == 0:
                    continue
                for half in ((0, 1) if d_z == 3 and self.core == 0 else (None,)):
                    ref = self.slot(*self.piece(d_z, d_k), half)
                    sem = self.share((d_z * 2 + d_k) * 2 + (half or 0))
                    remote(ref, ref, self.ici_sem, sem, self.place.at()).wait_recv()

    def sent(self, seven):
        remote(seven, seven, self.ici_sem, self.arrive(0), self.place.at()).wait_send()
        remote(seven, seven, self.d2d_sem, self.arrive(0), self.place.at()).wait_send()


class ByCore:
    def __init__(self, tag, place, gathers):
        self.tag, self.place, self.gathers = tag, place, gathers

    def step(self, name):
        for core in range(2):
            @pl.when(self.place.core == core)
            def _():
                with jax.named_scope(f'{self.tag}_{name}'):
                    getattr(self.gathers[core], name)()

    def shared(self):
        for core in range(2):
            @pl.when(self.place.core == core)
            def _():
                with jax.named_scope(f'{self.tag}_shared'):
                    self.gathers[1 - core].shared()

    def sent(self, sevens):
        for core in range(2):
            @pl.when(self.place.core == core)
            def _():
                self.gathers[core].sent(sevens[core])


def main_kernel(n_stage, x_ref, g_ref, wu_ref, wd_ref, y_ref, dx_ref, h_all, g_all, b1_ref, b2_ref,
                w1, w2, zb, act, hb, gb, ho, go,
                load_sem, mate_sem, mate_send, twin_sem, twin_send, arrive, share, ici, d2d,
                keep_sem, own_sem, own_send, blk_sem,
                xr, xs, gr, gs, fr, fs, br, bs, yr, ys, dr, ds):
    place = Place(n_stage)
    core, role, level = place.core, place.role, place.level
    first, last = level == 0, level == n_stage - 1
    n_blk, n_tile, f_blk = w1.shape[1:4]
    d_model = n_tile * f_blk
    tok = x_ref.shape[1]
    n_chunk = hb.shape[1]
    own_slot = place.z * SIDE + place.key * 2 + place.column
    mate_slot = place.z * SIDE + place.key * 2 + 1 - place.column
    matched = core == role
    twin = place.at(core=1 - core)

    @pl.when(matched)
    def _():
        for v in range(2):
            for k in range(n_tile):
                part = pl.ds(k * f_blk, f_blk)
                pltpu.make_async_copy(wu_ref.at[v, 0, part], w1.at[v, own_slot, k], load_sem.at[v, 0]).start()
                pltpu.make_async_copy(wd_ref.at[v, 0, :, part], w2.at[v, own_slot, k], load_sem.at[v, 1]).start()

    barrier = pltpu.get_barrier_semaphore()
    peers = [twin, place.at(y=place.pair_y), place.at(z=place.z_off(1)), place.at(z=place.z_off(-1)),
             place.at(y=place.mate_y, core=1 - core)]
    for off in range(place.n_x):
        x = lax.rem(place.x + off, place.n_x)
        peers.append(place.at(x=x, y=place.mate_y))
        if off:
            peers.append(place.at(x=x))
    for peer in peers:
        pl.semaphore_signal(barrier, inc=1, device_id=peer, device_id_type=MESH)
    with jax.named_scope('barrier'):
        pl.semaphore_wait(barrier, len(peers))

    @pl.when(jnp.logical_not(matched))
    def _():
        for v in range(2):
            for k in range(n_tile):
                part = pl.ds(k * f_blk, f_blk)
                remote(wu_ref.at[v, 0, part], w1.at[v, own_slot, k], mate_send.at[v, 0], mate_sem.at[v],
                       place.at(y=place.mate_y, core=0)).start()
                remote(wd_ref.at[v, 0, :, part], w2.at[v, own_slot, k], mate_send.at[v, 1], mate_sem.at[v],
                       place.at(y=place.mate_y, core=1)).start()

    def own_blocks(v):
        @pl.when(matched)
        def _():
            for colour, buf in enumerate((w1, w2)):
                ref = buf.at[v, own_slot]
                remote(ref, ref, twin_send.at[0, 0, 0], load_sem.at[v, colour], twin).wait_recv()
                remote(ref, ref, twin_send.at[v, colour, 0], twin_sem.at[v, colour, 0], twin).start()

        @pl.when(jnp.logical_not(matched))
        def _():
            for colour, buf in enumerate((w1, w2)):
                ref = buf.at[v, own_slot]
                remote(ref, ref, twin_send.at[0, 0, 0], twin_sem.at[v, colour, 0], twin).wait_recv()

        for colour, buf in enumerate((w1, w2)):
            @pl.when(core == colour)
            def _():
                ref = buf.at[v, mate_slot]
                remote(ref, ref, twin_send.at[0, 0, 0], mate_sem.at[v], twin).wait_recv()
                remote(ref, ref, twin_send.at[v, colour, 1], twin_sem.at[v, colour, 1], twin).start()

    def weights_of(v):
        gathers = []
        for colour, buf in enumerate((w1, w2)):
            def slot(z, key, half, buf=buf):
                base = z * SIDE + key * 2
                return buf.at[v, pl.ds(base, 2)] if half is None else buf.at[v, pl.ds(base + half, 1)]

            gathers.append(Gather(place, colour, slot, functools.partial(slot, place.z, place.key),
                                  lambda k: arrive.at[v, k], lambda k: share.at[v, k], ici.at[v], d2d.at[v]))
        return ByCore(f'w{v}', place, gathers)

    def lanes_of(tag, unit, buf, out, v, base, count):
        gathers = []
        for colour in range(2):
            def part(half):
                return pl.ds(base, count) if half is None else pl.ds(base + half * (count // 2), count // 2)

            def slot(z, key, half, colour=colour):
                return out.at[v, colour, z * 2 + key, part(half)]

            gathers.append(Gather(place, colour, slot, lambda half: buf.at[v, part(half)],
                                  lambda k: arrive.at[unit, k], lambda k: share.at[unit, k], ici.at[unit], d2d.at[unit]))
        return ByCore(tag, place, gathers)

    half_lane = n_chunk // 2
    weights = [weights_of(0), weights_of(1)]

    def weights_here(v):
        weights[v].shared()
        for colour, buf in enumerate((w1, w2)):
            @pl.when(core != colour)
            def _():
                ref = buf.at[v, mate_slot]
                remote(ref, ref, twin_send.at[0, 0, 0], twin_sem.at[v, colour, 1], twin).wait_recv()
    h0 = lanes_of('h0', 2, hb, h_all, 0, 0, n_chunk)
    h1 = lanes_of('h1', 3, hb, h_all, 1, 0, n_chunk)
    g1 = lanes_of('g1', 4, gb, g_all, 1, 0, n_chunk)
    g0a = lanes_of('g0a', 5, gb, g_all, 0, 0, half_lane)
    g0b = lanes_of('g0b', 6, gb, g_all, 0, half_lane, half_lane)

    def keep(k, v, base, count):
        buf, out = ((hb, h_all), (gb, g_all))[k]
        idx = 0 if base == 0 else 1
        part = pl.ds(base, count)
        for colour in range(2):
            @pl.when(core == colour)
            def _():
                dst = out.at[v, colour, place.z * 2 + place.key, part]
                pltpu.make_async_copy(buf.at[v, part], dst, keep_sem.at[k, v, idx]).start()
                remote(buf.at[v, part], dst, own_send.at[k, v, idx], own_sem.at[k, v, idx], twin).start()

    def kept(k, v, base, count):
        buf, out = ((hb, h_all), (gb, g_all))[k]
        idx = 0 if base == 0 else 1
        part = pl.ds(base, count)
        for colour in range(2):
            @pl.when(core == colour)
            def _():
                mine = out.at[v, colour, place.z * 2 + place.key, part]
                other = out.at[v, 1 - colour, place.z * 2 + place.key, part]
                pltpu.make_async_copy(buf.at[v, part], mine, keep_sem.at[k, v, idx]).wait()
                remote(buf.at[v, part], other, own_send.at[k, v, idx], own_sem.at[k, v, idx], twin).wait()

    micro = 2 * place.x + place.column
    x_dst, g_dst = hb.at[0, micro], gb.at[1, micro]

    @pl.when(first)
    def _():
        pltpu.make_async_copy(x_ref.at[0], x_dst, xr.at[micro]).start()

    @pl.when(jnp.logical_not(first))
    def _():
        remote(x_ref.at[0], x_dst, xs.at[0], xr.at[micro], place.at(x=0, y=place.key)).start()

    @pl.when(last)
    def _():
        pltpu.make_async_copy(g_ref.at[0], g_dst, gr.at[micro]).start()

    @pl.when(jnp.logical_not(last))
    def _():
        remote(g_ref.at[0], g_dst, gs.at[0], gr.at[micro], place.at(x=place.n_x - 1, y=place.key)).start()

    own_blocks(0)
    weights[0].step('start')
    own_blocks(1)
    weights[0].step('near')
    weights[1].step('start')
    weights[0].step('relay')
    weights[1].step('near')
    weights[0].step('last')
    weights_here(0)

    def wait_in(buf, v, m, ready, micro_ready, from_tokens):
        ref = buf.at[v, m]

        @pl.when(from_tokens)
        def _():
            remote(ref, ref, xs.at[0], micro_ready.at[m], twin).wait_recv()

        @pl.when(jnp.logical_not(from_tokens))
        def _():
            remote(ref, ref, xs.at[0], ready.at[v, m], twin).wait_recv()

    def give_out(src, m, out_ref, sends, recv):
        home_x = lax.div(m, 2)
        home_y = jnp.where(lax.rem(m, 2) == 0, place.key, 3 - place.key)
        here = (home_x == place.x) & (home_y == place.y)

        @pl.when(here)
        def _():
            pltpu.make_async_copy(src, out_ref.at[0], recv.at[0]).start()

        @pl.when(jnp.logical_not(here))
        def _():
            remote(src, out_ref.at[0], sends.at[m], recv.at[0], place.at(x=home_x, y=home_y)).start()

    up_x = lax.rem(place.x + role, place.n_x)
    up_y = jnp.where(role == 0, place.mate_y, place.y)
    down_x = lax.rem(place.x + place.n_x - 1 + role, place.n_x)
    down_y = jnp.where(role == 1, place.mate_y, place.y)

    def forward(v, m):
        with jax.named_scope('f_wait'):
            wait_in(hb, v, m, fr, xr, first & (v == 0))
        h_in = hb[v, m]
        for blk in range(n_blk):
            cols = slice(blk * f_blk, (blk + 1) * f_blk)
            pre_act = jnp.dot(h_in, w1[v, blk].reshape(d_model, f_blk), preferred_element_type=F32)
            zb[v, m, :, cols] = pre_act
            normal_cdf = 0.5 * (1.0 + lax.erf(pre_act * 0.7071067811865476))
            act[:, cols] = (pre_act * normal_cdf).astype(BF16)
        for k in range(n_tile):
            cols = slice(k * f_blk, (k + 1) * f_blk)
            branch = jnp.dot(act[...], w2[v, :, k].reshape(n_blk * f_blk, f_blk), preferred_element_type=F32)
            ho[v, m, :, cols] = (hb[v, m, :, cols].astype(F32) + branch).astype(BF16)
        done = last & (v == 1)

        @pl.when(done)
        def _():
            give_out(ho.at[v, m], m, y_ref, ys, yr)

        @pl.when(jnp.logical_not(done))
        def _():
            v_to = v + last.astype(jnp.int32)
            remote(ho.at[v, m], hb.at[v_to, m], fs.at[v, m], fr.at[v_to, m], place.at(x=up_x, y=up_y)).start()

    def transpose(v):
        for u in range(2):
            @pl.when(v == u)
            def _():
                for colour, (buf, out) in enumerate(((w1, b1_ref), (w2, b2_ref))):
                    mine = jnp.where(matched, own_slot, mate_slot)
                    copy = pltpu.make_async_copy(buf.at[u, mine], out.at[u], blk_sem.at[u, colour])
                    copy.start()
                weights[u].sent((w1.at[u, pl.ds(0, 14)], w2.at[u, pl.ds(0, 14)]))
                for colour, (buf, out) in enumerate(((w1, b1_ref), (w2, b2_ref))):
                    @pl.when(matched)
                    def _():
                        ref = buf.at[u, own_slot]
                        remote(ref, ref, twin_send.at[u, colour, 0], twin_sem.at[u, colour, 0], twin).wait_send()

                    @pl.when(core == colour)
                    def _():
                        ref = buf.at[u, mate_slot]
                        remote(ref, ref, twin_send.at[u, colour, 1], twin_sem.at[u, colour, 1], twin).wait_send()

                    pltpu.make_async_copy(buf.at[u, own_slot], out.at[u], blk_sem.at[u, colour]).wait()

        def tiles(blk, carry):
            for buf in (w2, w1):
                for k in range(n_tile):
                    buf[v, blk, k] = buf[v, blk, k].T
            return carry

        with jax.named_scope('transpose'):
            lax.fori_loop(0, n_blk, tiles, 0)

    def backward(v, m):
        with jax.named_scope('b_wait'):
            wait_in(gb, v, m, br, gr, last & (v == 1))
        g_out = gb[v, m]
        for blk in range(n_blk):
            cols = slice(blk * f_blk, (blk + 1) * f_blk)
            d_act = jnp.dot(g_out, w2[v, blk].reshape(d_model, f_blk), preferred_element_type=F32)
            pre_act = zb[v, m, :, cols]
            normal_cdf, normal_pdf = gelu_parts(pre_act)
            act[:, cols] = (d_act * (normal_cdf + pre_act * normal_pdf)).astype(BF16)
        for k in range(n_tile):
            cols = slice(k * f_blk, (k + 1) * f_blk)
            back = jnp.dot(act[...], w1[v, :, k].reshape(n_blk * f_blk, f_blk), preferred_element_type=F32)
            go[v, m, :, cols] = (gb[v, m, :, cols].astype(F32) + back).astype(BF16)
        done = first & (v == 0)

        @pl.when(done)
        def _():
            give_out(go.at[v, m], m, dx_ref, ds, dr)

        @pl.when(jnp.logical_not(done))
        def _():
            v_to = v - first.astype(jnp.int32)
            remote(go.at[v, m], gb.at[v_to, m], bs.at[v, m], br.at[v_to, m], place.at(x=down_x, y=down_y)).start()

    f0 = level
    b0 = 2 * n_stage + n_chunk - 1 + (n_stage - 1 - level)
    f1, b1 = f0 + n_stage, b0 + n_stage

    def tick(t, carry):
        f_pos = jnp.maximum(t - f0, 0)
        f_v, f_m = lax.div(f_pos, n_stage), lax.rem(f_pos, n_stage)
        f_on = (t >= f0) & (f_v < 2) & (f_m < n_chunk)
        b_pos = jnp.maximum(t - b0, 0)
        b_k, b_m = lax.div(b_pos, n_stage), lax.rem(b_pos, n_stage)
        b_on = (t >= b0) & (b_k < 2) & (b_m < n_chunk)

        def at(when, *steps):
            @pl.when(t == when)
            def _():
                for step in steps:
                    step()

        at(f1,
           lambda: weights[1].step('relay'),
           lambda: transpose(0),
           lambda: weights[1].step('last'),
           lambda: weights_here(1),
           lambda: h0.step('start'),
           lambda: keep(0, 0, 0, n_chunk))
        at(b1,
           lambda: g1.step('start'),
           lambda: keep(1, 1, 0, n_chunk),
           lambda: g1.step('near'))

        @pl.when(f_on)
        def _():
            forward(f_v, f_m)

        at(f1 + n_chunk - 1, lambda: transpose(1))

        @pl.when(b_on)
        def _():
            backward(1 - b_k, b_m)

        at(f1 + n_chunk // 2, lambda: h0.step('near'))
        at(f1 + n_chunk,
           lambda: h0.step('relay'),
           lambda: h1.step('start'),
           lambda: keep(0, 1, 0, n_chunk))
        at(f1 + n_chunk + n_chunk // 2, lambda: h0.step('last'), lambda: h1.step('near'))
        at(f1 + 2 * n_chunk - 1, lambda: h1.step('relay'))
        at(b1 + n_chunk // 2 - 1, lambda: g1.step('relay'), lambda: h1.step('last'))
        at(b1 + n_chunk // 2, lambda: g0a.step('start'), lambda: keep(1, 0, 0, half_lane))
        at(b1 + n_chunk - 1,
           lambda: g0a.step('near'),
           lambda: g0b.step('start'),
           lambda: keep(1, 0, half_lane, half_lane),
           lambda: g1.step('last'),
           lambda: g0a.step('relay'),
           lambda: g0b.step('near'),
           lambda: g0a.step('last'),
           lambda: g0b.step('relay'),
           lambda: g0b.step('last'))
        return carry

    lax.fori_loop(0, 4 * n_stage + 2 * n_chunk, tick, 0)

    for unit in (h0, h1, g1, g0a, g0b):
        unit.shared()
    for k, v, base, count in ((0, 0, 0, n_chunk), (0, 1, 0, n_chunk), (1, 1, 0, n_chunk),
                              (1, 0, 0, half_lane), (1, 0, half_lane, half_lane)):
        kept(k, v, base, count)
    seven = pl.ds(0, 7)
    for unit, out, v, part in ((h0, h_all, 0, pl.ds(0, n_chunk)), (h1, h_all, 1, pl.ds(0, n_chunk)), (g1, g_all, 1, pl.ds(0, n_chunk)),
                               (g0a, g_all, 0, pl.ds(0, half_lane)), (g0b, g_all, 0, pl.ds(half_lane, half_lane))):
        unit.sent((out.at[v, 0, seven, part], out.at[v, 1, seven, part]))

    def wait_sent(ref, sem):
        remote(ref, ref, sem, xr.at[0], twin).wait_send()

    @pl.when(jnp.logical_not(matched))
    def _():
        for v in range(2):
            for colour, buf in enumerate((w1, w2)):
                wait_sent(buf.at[v, 0], mate_send.at[v, colour])

    @pl.when(jnp.logical_not(first))
    def _():
        wait_sent(x_ref.at[0], xs.at[0])

    @pl.when(jnp.logical_not(last))
    def _():
        wait_sent(g_ref.at[0], gs.at[0])

    for m in range(n_chunk):
        home_x = m // 2
        home_y = jnp.where(m % 2 == 0, place.key, 3 - place.key)
        here = (home_x == place.x) & (home_y == place.y)
        for v in range(2):
            ends, starts = last & (v == 1), first & (v == 0)

            @pl.when(jnp.logical_not(ends))
            def _():
                wait_sent(ho.at[v, m], fs.at[v, m])

            @pl.when(jnp.logical_not(starts))
            def _():
                wait_sent(go.at[v, m], bs.at[v, m])

        @pl.when(last & jnp.logical_not(here))
        def _():
            wait_sent(ho.at[1, m], ys.at[m])

        @pl.when(first & jnp.logical_not(here))
        def _():
            wait_sent(go.at[0, m], ds.at[m])

    remote(y_ref.at[0], y_ref.at[0], xs.at[0], yr.at[0], twin).wait_recv()
    remote(dx_ref.at[0], dx_ref.at[0], xs.at[0], dr.at[0], twin).wait_recv()


def grad_kernel(n_stage, h_ref, g_ref, b1_ref, b2_ref, du_ref, dd_ref, acc_u, acc_d, out_u, send_sem, recv_sem):
    place = Place(n_stage)
    mate = place.at(y=place.mate_y, core=1 - place.core)
    matched = place.core == place.role
    group, step = 1 - pl.program_id(0), pl.program_id(1)
    end = pl.num_programs(1) - 1
    n_tile, f_blk = b1_ref.shape[1:3]
    d_model = n_tile * f_blk
    rows = h_ref.shape[1] * h_ref.shape[2] * h_ref.shape[3]

    @pl.when((group == 1) & (step == 0))
    def _():
        barrier = pltpu.get_barrier_semaphore()
        pl.semaphore_signal(barrier, inc=1, device_id=mate, device_id_type=MESH)
        pl.semaphore_wait(barrier, 1)

    @pl.when(step == 0)
    def _():
        acc_u[...] = jnp.zeros_like(acc_u)
        acc_d[group] = jnp.zeros_like(acc_d[group])

    h_in = h_ref[...].reshape(rows, d_model)
    g_out = g_ref[...].reshape(rows, d_model)
    pre_act = jnp.dot(h_in, b1_ref[0].reshape(d_model, f_blk), preferred_element_type=F32)
    d_act = None
    for k in range(n_tile):
        term = lax.dot_general(g_out[:, k * f_blk:(k + 1) * f_blk], b2_ref[0, k], NT, preferred_element_type=F32)
        d_act = term if d_act is None else d_act + term
    normal_cdf, normal_pdf = gelu_parts(pre_act)
    act_val = (pre_act * normal_cdf).astype(BF16)
    d_pre = (d_act * (normal_cdf + pre_act * normal_pdf)).astype(BF16)
    acc_u[...] += lax.dot_general(d_pre, h_in, TN, preferred_element_type=F32)
    acc_d[group] += lax.dot_general(act_val, g_out, TN, preferred_element_type=F32)

    def give(v, start):
        for k, (src, dst) in enumerate(((acc_d.at[v], dd_ref.at[v, 0]), (out_u.at[v], du_ref.at[v, 0]))):
            @pl.when(matched)
            def _():
                copy = pltpu.make_async_copy(src, dst, recv_sem.at[v, k])
                copy.start() if start else copy.wait()

            @pl.when(jnp.logical_not(matched))
            def _():
                copy = remote(src, dst, send_sem.at[v, k], recv_sem.at[v, k], mate)
                copy.start() if start else copy.wait()

    for v in range(2):
        @pl.when((group == v) & (step == end))
        def _():
            out_u[v] = acc_u[...].T
            give(v, True)

    @pl.when((group == 0) & (step == end))
    def _():
        for v in range(2):
            give(v, False)


def solution(mesh):
    n_stage = mesh.shape['stage']
    n_inner = mesh.shape['inner']
    tok_spec = P(('data', 'stage', 'inner'))
    up_spec = P(None, ('data', 'stage'), None, 'inner')
    down_spec = P(None, ('data', 'stage'), 'inner', None)

    def device_step(x_loc, g_loc, w_up, w_down):
        tok, d_model = x_loc.shape[1:]
        f_blk = w_up.shape[3]
        n_tile = d_model // f_blk
        n_chunk = n_stage
        f_full = n_inner * f_blk
        any_spec = pl.BlockSpec(memory_space=pl.ANY)
        dma = pltpu.SemaphoreType.DMA
        lanes = jax.ShapeDtypeStruct((2, 2, n_inner // 2, n_chunk, tok, d_model), BF16)
        blocks = jax.ShapeDtypeStruct((2, n_tile, f_blk, f_blk), BF16)
        y_loc, dx_loc, h_all, g_all, b1, b2 = pl.pallas_call(
            functools.partial(main_kernel, n_stage),
            name='stack',
            out_shape=(jax.ShapeDtypeStruct(x_loc.shape, BF16), jax.ShapeDtypeStruct(x_loc.shape, BF16),
                       lanes, lanes, blocks, blocks),
            in_specs=[any_spec] * 4,
            out_specs=(any_spec,) * 6,
            scratch_shapes=[
                pltpu.VMEM((2, n_inner, n_tile, f_blk, f_blk), BF16),
                pltpu.VMEM((2, n_inner, n_tile, f_blk, f_blk), BF16),
                pltpu.VMEM((2, n_chunk, tok, f_full), F32),
                pltpu.VMEM((tok, f_full), BF16),
                pltpu.VMEM((2, n_chunk, tok, d_model), BF16),
                pltpu.VMEM((2, n_chunk, tok, d_model), BF16),
                pltpu.VMEM((2, n_chunk, tok, d_model), BF16),
                pltpu.VMEM((2, n_chunk, tok, d_model), BF16),
                dma((2, 2)), dma((2,)), dma((2, 2)), dma((2, 2, 2)), dma((2, 2, 2)),
                dma((7, 16)), dma((7, 16)), dma((7,)), dma((7,)),
                dma((2, 2, 2)), dma((2, 2, 2)), dma((2, 2, 2)), dma((2, 2)),
                dma((n_chunk,)), dma((1,)), dma((n_chunk,)), dma((1,)),
                dma((2, n_chunk)), dma((2, n_chunk)), dma((2, n_chunk)), dma((2, n_chunk)),
                dma((1,)), dma((n_chunk,)), dma((1,)), dma((n_chunk,)),
            ],
            compiler_params=pltpu.CompilerParams(
                collective_id=0, has_side_effects=True, vmem_limit_bytes=60 << 20),
        )(x_loc, g_loc, w_up, w_down)

        h_all = h_all.reshape(2, n_inner, n_chunk, tok, d_model)
        g_all = g_all.reshape(2, n_inner, n_chunk, tok, d_model)
        lane_spec = pl.BlockSpec((1, 2, n_chunk, tok, d_model), lambda v, t: (1 - v, t, 0, 0, 0))
        block_spec = pl.BlockSpec((1, n_tile, f_blk, f_blk), lambda v, t: (1 - v, 0, 0, 0))
        dw_up, dw_down = pl.pallas_call(
            functools.partial(grad_kernel, n_stage),
            name='grads',
            grid=(2, n_inner // 2),
            out_shape=(jax.ShapeDtypeStruct(w_up.shape, F32), jax.ShapeDtypeStruct(w_down.shape, F32)),
            in_specs=[lane_spec, lane_spec, block_spec, block_spec],
            out_specs=(any_spec, any_spec),
            scratch_shapes=[pltpu.VMEM((f_blk, d_model), F32), pltpu.VMEM((2, f_blk, d_model), F32),
                            pltpu.VMEM((2, d_model, f_blk), F32), dma((2, 2)), dma((2, 2))],
            compiler_params=pltpu.CompilerParams(
                dimension_semantics=('arbitrary', 'arbitrary'), collective_id=1, has_side_effects=True,
                vmem_limit_bytes=40 << 20),
        )(h_all, g_all, b1, b2)
        return y_loc, dx_loc, dw_up, dw_down

    return jax.shard_map(device_step, mesh=mesh, in_specs=(tok_spec, tok_spec, up_spec, down_spec),
                         out_specs=(tok_spec, tok_spec, up_spec, down_spec), check_vma=False)
```
